128 devices in a mesh: blk: 8 (over y, z_lo), seg: 16 (over x, z_hi, core).
Axes of the slice: x: 4, y: 4, z: 4 (z_hi: 2, z_lo: 2; z = z_hi * 2 + z_lo), core: 2. Of those that a mesh axis runs over, the one named last changes fastest.
Arguments:
- spectra: bfloat16 [16, 2, 4096, 2048], P('seg', None, 'blk'), may hold values from -6 to 6
- window_count: int32 [16], P('seg'), may hold values from 1 to 2, as said below
- tile_owner: int32 [8, 80], P('blk'), may hold values from 0 to 15, as said below
- phases: float32 [2, 128, 256], replicated, may hold values from -3.140625 to 3.140625
Outputs:
- tile_power: float32 [8, 16, 8, 2, 256], P('blk', 'seg')
The draws below stay inside these ranges and needn't reach their ends.
Inputs may be any that keep to these rules, and one draw needn't show every extreme that they name: `window_count`: the largest value, 2, occurs in every draw. `tile_owner`: in each row no segment index occurs more than 8 times, and some index occurs exactly 8 times.
All inputs are finite; a program needn't handle non-finite values.
Results may differ from the reference program's by a relative error of at most 0.004.
Values may be sent and summed in bfloat16 or wider, within the bound.
A program may use at most 128 MiB of HBM per device.

```python
import math
import jax
import jax.numpy as jnp
from jax import lax

CH_DEV = 512
TILE = 128
FREQ = 1024
BANDS = 2
VEL = 256
CAP = 8
WIN = 2
FB = 512
SEGS = 16
BLOCKS = 8
CHANNELS = 4096
QUAD = 4
TCOL = 80


def draw_window_count(key, part):
    first_key, second_key = jax.random.split(jax.random.fold_in(key, 11))
    counted = jax.random.randint(first_key, (SEGS,), 1, WIN + 1)
    chosen = jax.random.randint(second_key, (), 0, SEGS)
    return jnp.where(jnp.arange(SEGS) == chosen, WIN, counted).astype(jnp.int32)


def draw_tile_owner(key, part):
    slot_count = SEGS * CAP

    def one_column(column_key):
        first_key, second_key, third_key = jax.random.split(column_key, 3)
        order_ids = jax.random.permutation(first_key, slot_count)
        position = jnp.argsort(order_ids)
        full_owner = jax.random.randint(second_key, (), 0, SEGS)
        score = position + jnp.where(jnp.arange(slot_count) // CAP == full_owner, 0, slot_count)
        chosen = jnp.argsort(score)[:TCOL]
        tile_perm = jax.random.permutation(third_key, TCOL)
        owners = jnp.zeros((TCOL,), jnp.int32).at[tile_perm].set((chosen // CAP).astype(jnp.int32))
        return owners
    column_keys = jax.random.split(jax.random.fold_in(key, 23), BLOCKS)
    return jax.vmap(one_column)(column_keys).astype(jnp.int32)


def levels(own_key, shape, cuts, smallest, top_value):
    loudness, own = 1.0, jax.random.fold_in(own_key, 6)
    for dim, shards_of in cuts:
        draws = jnp.exp(jax.random.uniform(jax.random.fold_in(own, dim), (shards_of,), jnp.float32, smallest / len(cuts), top_value / len(cuts)))
        loudness = loudness * jnp.repeat(draws, shape[dim] // shards_of).reshape([-1 if axis == dim else 1 for axis in range(len(shape))])
    return loudness


def bell_draw(rng, extent, scale, reach, shards=(), held_as=jnp.bfloat16):
    factor_of = levels(rng, extent, shards, -0.22, 0.18) if shards else 1.0
    result = jax.random.normal(rng, extent, jnp.float32) * scale * factor_of
    return jnp.minimum(jnp.maximum(result, -reach), reach).astype(held_as)


def setup_inputs(seed: int = 0) -> dict:
    seeds = jax.random.split(jax.random.key(seed), 5)
    spectra = bell_draw(seeds[0], (SEGS, WIN, CHANNELS, 2 * FREQ), 1.0, 6.0, ((0, 16), (2, 8)))
    window_count = draw_window_count(jax.random.fold_in(seeds[4], 71), 0)
    tile_owner = draw_tile_owner(jax.random.fold_in(seeds[4], 71), 0)
    phases = jnp.clip(jax.random.uniform(seeds[3], (BANDS, TILE, VEL), jnp.float32, -3.140625, 3.140625), -3.140625, 3.140625)
    return {"spectra": spectra, "window_count": window_count, "tile_owner": tile_owner, "phases": phases}


def prepare(segment_data, counted):
    spectrum = segment_data.astype(jnp.float32).reshape(WIN, CHANNELS, BANDS, 2, FB)
    scaling = lax.rsqrt(lax.optimization_barrier(jnp.mean(spectrum * spectrum, axis=(2, 3, 4))) + 1e-05)
    live_mask = (jnp.arange(WIN, dtype=jnp.int32) < counted).astype(jnp.float32)
    return (spectrum * scaling[:, :, None, None, None] * live_mask[:, None, None, None, None]).astype(jnp.bfloat16)

def correlate(resident, visiting, weight):
    flipped = jnp.stack([-visiting[:, :, :, 1], visiting[:, :, :, 0]], axis=3)
    both_parts = jnp.stack([visiting, flipped], axis=1)
    left_side = resident.astype(jnp.float32).reshape(WIN, QUAD, TILE, BANDS, 2 * FB)
    right_side = both_parts.astype(jnp.float32).reshape(WIN, 2, QUAD, TILE, BANDS, 2 * FB)
    product = jnp.einsum('wqibk,wpsjbk->qsbipj', left_side, right_side, precision=lax.Precision.HIGHEST)
    return (product * weight).astype(jnp.bfloat16).reshape(QUAD * QUAD, BANDS, TILE, 2 * TILE)

def disperse(stacked, phases):
    norm_factor = 1.0 / math.sqrt(TILE)
    cosine = (jnp.cos(phases) * norm_factor).astype(jnp.bfloat16)
    sine_part = (jnp.sin(phases) * norm_factor).astype(jnp.bfloat16)
    upper = jnp.concatenate([cosine, sine_part], axis=2)
    lower = jnp.concatenate([-sine_part, cosine], axis=2)
    matrix = jnp.concatenate([upper, lower], axis=1).astype(jnp.float32)
    field = jnp.einsum('nbij,bjv->nbiv', stacked.astype(jnp.float32), matrix, precision=lax.Precision.HIGHEST)
    squared = field * field
    energy = squared[..., :VEL] + squared[..., VEL:]
    return lax.optimization_barrier(jnp.mean(energy, axis=2))

def slot_table(owner_row, segments):
    count_tiles = owner_row.shape[0]
    order_ids = jnp.arange(count_tiles, dtype=jnp.int32)
    same_owner = owner_row[:, None] == owner_row[None, :]
    earlier = order_ids[None, :] < order_ids[:, None]
    rank_of = lax.optimization_barrier(jnp.sum(jnp.where(same_owner & earlier, 1, 0), axis=1)).astype(jnp.int32)
    slot_ids = owner_row * CAP + rank_of
    grid_ids = jnp.arange(segments * CAP, dtype=jnp.int32)
    matches = grid_ids[:, None] == slot_ids[None, :]
    tile_of_slot = lax.optimization_barrier(jnp.sum(jnp.where(matches, order_ids[None, :], 0), axis=1)).astype(jnp.int32)
    filled = jnp.any(matches, axis=1)
    return (tile_of_slot, filled)

def reference(spectra, window_count, tile_owner, phases):

    def one_block(block_index):

        def add_segment(segment, running):
            segment_data = lax.dynamic_index_in_dim(spectra, segment, 0, keepdims=False)
            counted = lax.dynamic_index_in_dim(window_count, segment, 0, keepdims=False)
            whitened = prepare(segment_data, counted)
            weight = 1.0 / (counted.astype(jnp.float32) * math.sqrt(FB * SEGS))
            resident = lax.dynamic_slice_in_dim(whitened, (block_index * CH_DEV).astype(jnp.int32), CH_DEV, 1)
            pieces = []
            for shift_step in range(BLOCKS // 2 + 1):
                start = ((block_index + shift_step) % BLOCKS * CH_DEV).astype(jnp.int32)
                visiting = lax.dynamic_slice_in_dim(whitened, start, CH_DEV, 1)
                pieces.append(correlate(resident, visiting, weight))
            return running + jnp.concatenate(pieces, axis=0).astype(jnp.float32)
        initial = jnp.zeros((TCOL, BANDS, TILE, 2 * TILE), jnp.float32)
        stacked = lax.fori_loop(0, SEGS, add_segment, initial).astype(jnp.bfloat16)
        powers = disperse(stacked, phases)
        owner_row = lax.dynamic_index_in_dim(tile_owner, block_index, 0, keepdims=False)
        tile_of_slot, filled = slot_table(owner_row, SEGS)
        placed = jnp.take(powers, tile_of_slot, axis=0) * filled[:, None, None].astype(jnp.float32)
        return placed.reshape(SEGS, CAP, BANDS, VEL)
    return lax.map(one_block, jnp.arange(BLOCKS, dtype=jnp.int32))
```

```python
import math

import jax
import jax.numpy as jnp
from jax import lax
from jax.experimental import pallas as pl
from jax.experimental.pallas import tpu as pltpu
from jax.sharding import PartitionSpec as P

TILE = 128
BANDS = 2
CAP = 8
FB = 512
QUAD = 4
ROUNDS = 10
PART = 2 * FB
MESH = pl.DeviceIdType.MESH


def pick(index, values):
    total = 0
    for key, value in enumerate(values):
        total = total + jnp.where(index == key, value, 0)
    return total


def kernel(
    rows_ref, filled_ref, scale_ref, spectra_ref, phases_ref, out_ref,
    raw, zs, data, out, core_in, relay_in, ring_in, zhi_in, zhi_out, keep,
    phase, matrix, powers, gathered,
    raw_sem, phase_sem, z_sem, up_sem, dn_sem, core_sem, relay_sem, ring_sem, zhi_sem,
    near_send, near_recv, far_send, far_recv,
):
    blk = lax.axis_index("blk")
    seg = lax.axis_index("seg")
    y, zl = blk // 2, blk % 2
    x, zh, core = seg // 4, (seg // 2) % 2, seg % 2
    first, second = zl, 1 - zl
    left, right = (x + 3) % 4, (x + 1) % 4

    def seat(nx, nzh, nc):
        return nx * 4 + nzh * 2 + nc

    def remote(src, dst, sems, index, device):
        return pltpu.make_async_remote_copy(
            src_ref=src, dst_ref=dst,
            send_sem=sems.at[(0,) + index], recv_sem=sems.at[(1,) + index],
            device_id=device, device_id_type=MESH,
        )

    def z_copy(j):
        return remote(zs.at[j], data.at[2 * zl, j], z_sem, (j,), (2 * y + 1 - zl, seg))

    def z_wait(j):
        remote(zs.at[j], data.at[2 * second, j], z_sem, (j,), (2 * y + 1 - zl, seg)).wait_recv()

    def up_copy(p, j):
        return remote(data.at[2 * p, j], data.at[8 + p, j], up_sem, (p, j), (2 * ((y + 3) % 4) + zl, seg))

    def dn_copy(p, j):
        return remote(data.at[2 * p, j], data.at[4 + 2 * p, j], dn_sem, (p, j), (2 * ((y + 1) % 4) + zl, seg))

    def core_copy(n):
        return remote(
            out.at[n, pl.ds(2 * (1 - core), 2)], core_in.at[n], core_sem, (n,),
            (blk, seat(x, zh, 1 - core)),
        )

    def relay_copy(n, side):
        return remote(
            out.at[n, 2 * core + side, (x + 2) % 4], relay_in.at[n, side], relay_sem, (n, side),
            (blk, seat(right if side else left, zh, core)),
        )

    def ring_copy(n, side):
        to = right if side else left
        return remote(
            out.at[n, pl.ds(2 * core, 2), to], ring_in.at[n, side], ring_sem, (n, side),
            (blk, seat(to, zh, core)),
        )

    def zhi_copy(n):
        return remote(zhi_out.at[n], zhi_in.at[n], zhi_sem, (n,), (blk, seat(x, 1 - zh, core)))

    me = zl * 16 + seg

    def near_copy(i):
        return pltpu.make_async_remote_copy(
            src_ref=powers.at[pl.ds(0, 8)],
            dst_ref=gathered.at[pl.ds(pl.multiple_of(me * 8, 8), 8)],
            send_sem=near_send.at[i], recv_sem=near_recv.at[me],
            device_id=(2 * y + (zl + i // 16) % 2, (seg + i % 16) % 16), device_id_type=MESH,
        )

    def near_wait(i):
        other = ((zl + i // 16) % 2) * 16 + (seg + i % 16) % 16
        pltpu.make_async_remote_copy(
            src_ref=powers.at[pl.ds(0, 8)],
            dst_ref=gathered.at[pl.ds(pl.multiple_of(other * 8, 8), 8)],
            send_sem=near_send.at[i], recv_sem=near_recv.at[other],
            device_id=(2 * y + (zl + i // 16) % 2, (seg + i % 16) % 16), device_id_type=MESH,
        ).wait_recv()

    def far_copy(i):
        return pltpu.make_async_remote_copy(
            src_ref=powers.at[pl.ds(8, 8)],
            dst_ref=gathered.at[pl.ds(pl.multiple_of((32 + me) * 8, 8), 8)],
            send_sem=far_send.at[i], recv_sem=far_recv.at[me],
            device_id=(2 * ((y + 3) % 4) + (zl + i // 16) % 2, (seg + i % 16) % 16),
            device_id_type=MESH,
        )

    def far_wait(i):
        pltpu.make_async_remote_copy(
            src_ref=powers.at[pl.ds(8, 8)],
            dst_ref=gathered.at[pl.ds(pl.multiple_of((32 + i) * 8, 8), 8)],
            send_sem=far_send.at[i], recv_sem=far_recv.at[i],
            device_id=(2 * ((y + 3) % 4) + i // 16, i % 16), device_id_type=MESH,
        ).wait_recv()

    def each(count, action):
        def step(i, carry):
            action(i)
            return carry

        lax.fori_loop(0, count, step, 0)

    def raw_copy(j):
        return pltpu.make_async_copy(
            spectra_ref.at[:, pl.ds(pl.multiple_of(j * TILE, TILE), TILE), :], raw.at[j], raw_sem.at[j]
        )

    phase_copy = pltpu.make_async_copy(phases_ref.at[zl], phase, phase_sem.at[0])
    for j in range(QUAD):
        raw_copy(j).start()
    phase_copy.start()

    def whiten(j):
        raw_copy(j).wait()

        def some_rows(r):
            rows = pl.ds(pl.multiple_of(r * 16, 16), 16)
            for w in range(2):
                mine = raw[j, w, rows, pl.ds(pl.multiple_of(zl * PART, PART), PART)].astype(jnp.float32)
                theirs = raw[j, w, rows, pl.ds(pl.multiple_of(second * PART, PART), PART)].astype(jnp.float32)
                square = jnp.sum(mine * mine + theirs * theirs, axis=1, keepdims=True)
                scaling = lax.rsqrt(square * (1.0 / (2 * PART)) + 1e-05) * scale_ref[1 + w]
                mine = (mine * scaling).astype(jnp.bfloat16)
                data[2 * zl, j, rows, w * PART : (w + 1) * PART] = mine
                data[2 * zl + 1, j, rows, w * PART : w * PART + FB] = mine[:, FB:]
                data[2 * zl + 1, j, rows, w * PART + FB : (w + 1) * PART] = -mine[:, :FB]
                zs[j, rows, w * PART : (w + 1) * PART] = (theirs * scaling).astype(jnp.bfloat16)

        each(TILE // 16, some_rows)
        z_copy(j).start()
        up_copy(zl, j).start()
        dn_copy(zl, j).start()

    each(QUAD, whiten)

    def flip(slab, j):
        def some_rows(r):
            rows = pl.ds(pl.multiple_of(r * 16, 16), 16)
            for w in range(2):
                data[slab + 1, j, rows, w * PART : w * PART + FB] = data[slab, j, rows, w * PART + FB : (w + 1) * PART]
                data[slab + 1, j, rows, w * PART + FB : (w + 1) * PART] = -data[slab, j, rows, w * PART : w * PART + FB]

        each(TILE // 16, some_rows)

    phase_copy.wait()
    angles = phase[...]
    norm_factor = 1.0 / math.sqrt(TILE)
    cosine = (jnp.cos(angles) * norm_factor).astype(jnp.bfloat16)
    sine_part = (jnp.sin(angles) * norm_factor).astype(jnp.bfloat16)
    velocities = angles.shape[1]
    matrix[:TILE, :velocities] = cosine
    matrix[:TILE, velocities:] = sine_part
    matrix[TILE:, :velocities] = -sine_part
    matrix[TILE:, velocities:] = cosine
    powers[...] = jnp.zeros_like(powers)

    def job(n, h):
        @pl.when(n == 1)
        def _():
            for jj in range(2):
                j = 2 * h + jj
                z_wait(j)
                up_copy(second, j).start()
                dn_copy(second, j).start()
                flip(2 * second, j)
                up_copy(first, j).wait_recv()
                dn_copy(first, j).wait_recv()
                flip(4 + 2 * first, j)

        @pl.when(((n == 6) | (n == 7)) & (h == 0))
        def _():
            for jj in range(2):
                j = 2 * (n - 6) + jj
                up_copy(second, j).wait_recv()
                dn_copy(second, j).wait_recv()
                flip(4 + 2 * second, j)

        either = (zl + h) % 2
        left_slab = pick(n, [first, first, second, 0, second, 2 + first, either, either, 2 + second, 3])
        right_slab = pick(
            n, [2 * first, 8 + first, 2 * second, 2, 8 + first, 8 + first, 8 + second, 8 + second, 8 + second, 8]
        )
        pair = pick(n, [h, h, h, h, h, h, 0, 1, h, h])
        left_side = data[pl.ds(2 * left_slab, 2)].reshape(2 * QUAD * TILE, 2 * PART)
        right_side = data[right_slab, pl.ds(2 * pair, 2)].reshape(2 * TILE, 2 * PART)
        product = lax.dot_general(
            left_side, right_side, (((1,), (1,)), ((), ())), preferred_element_type=jnp.float32
        )
        product = (product * scale_ref[0]).astype(jnp.bfloat16).reshape(2, QUAD, TILE, 2 * TILE)
        for jj in range(2):
            columns = slice(jj * TILE, (jj + 1) * TILE)
            out[n, 2 * h + jj, :, :, :TILE] = product[0, :, :, columns]
            out[n, 2 * h + jj, :, :, TILE:] = product[1, :, :, columns]

    def add_cores(n):
        core_copy(n).wait_recv()

        def one(t):
            q, r = t // 4, t % 4
            total = out[n, 2 * core + q, r].astype(jnp.float32) + core_in[n, q, r].astype(jnp.float32)
            out[n, 2 * core + q, r] = total.astype(jnp.bfloat16)

        each(8, one)
        for side in range(2):
            relay_copy(n, side).start()

    def add_relayed(n):
        for side in range(2):
            to = right if side else left
            relay_copy(n, side).wait_recv()
            total = out[n, 2 * core + side, to].astype(jnp.float32) + relay_in[n, side].astype(jnp.float32)
            out[n, 2 * core + side, to] = total.astype(jnp.bfloat16)
        for side in range(2):
            ring_copy(n, side).start()

    def add_ring(n):
        for side in range(2):
            ring_copy(n, side).wait_recv()

        def total(z):
            return (
                out[n, 2 * core + z, x].astype(jnp.float32)
                + ring_in[n, 0, z].astype(jnp.float32)
                + ring_in[n, 1, z].astype(jnp.float32)
            )

        zhi_out[n] = total(1 - zh).astype(jnp.bfloat16)
        zhi_copy(n).start()
        keep[n] = total(zh)

    def add_last(n):
        zhi_copy(n).wait_recv()
        stacked = (keep[n] + zhi_in[n].astype(jnp.float32)).astype(jnp.bfloat16)
        field = jnp.dot(stacked, matrix[...], preferred_element_type=jnp.float32)
        squared = field * field
        energy = squared[:, :velocities] + squared[:, velocities:]
        power = jnp.sum(energy, axis=0, keepdims=True) * (1.0 / TILE)
        powers[pl.ds(n, 1), :] = power

        @pl.when(n == 5)
        def _():
            powers[10:11, :] = power

    def step(n):
        @pl.when(n < ROUNDS)
        def _():
            each(2, lambda h: job(n, h))
            core_copy(n).start()

        @pl.when((n >= 1) & (n <= ROUNDS))
        def _():
            add_cores(n - 1)

        @pl.when((n >= 2) & (n <= ROUNDS + 1))
        def _():
            add_relayed(n - 2)

        @pl.when((n >= 3) & (n <= ROUNDS + 2))
        def _():
            add_ring(n - 3)

        @pl.when(n >= 4)
        def _():
            add_last(n - 4)

    each(ROUNDS + 4, step)

    gathered[pl.ds(pl.multiple_of(me * 8, 8), 8), :] = powers[:8, :]
    each(31, lambda i: near_copy(i + 1).start())
    each(32, lambda i: far_copy(i).start())
    each(31, lambda i: near_wait(i + 1))
    each(32, far_wait)

    for c in range(CAP):
        for g in range(BANDS):
            row = gathered[pl.ds(rows_ref[c * BANDS + g], 1), :]
            out_ref[c, g : g + 1, :] = jnp.where(filled_ref[c] > 0, row, jnp.zeros_like(row))

    def drain_exchange(j):
        z_copy(j).wait_send()
        for p in range(2):
            up_copy(p, j).wait_send()
            dn_copy(p, j).wait_send()

    each(QUAD, drain_exchange)

    def drain_rounds(n):
        core_copy(n).wait_send()
        for side in range(2):
            relay_copy(n, side).wait_send()
            ring_copy(n, side).wait_send()
        zhi_copy(n).wait_send()

    each(ROUNDS, drain_rounds)
    each(31, lambda i: near_copy(i + 1).wait_send())
    each(32, lambda i: far_copy(i).wait_send())


def slot_rows(owner_row, block, segment):
    count_tiles = owner_row.shape[0]
    order_ids = jnp.arange(count_tiles, dtype=jnp.int32)
    mine = owner_row == segment
    earlier = order_ids[None, :] < order_ids[:, None]
    rank_of = jnp.sum(jnp.where(mine[None, :] & earlier, 1, 0), axis=1).astype(jnp.int32)
    slots = jnp.arange(CAP, dtype=jnp.int32)
    matches = mine[None, :] & (rank_of[None, :] == slots[:, None])
    tile = jnp.sum(jnp.where(matches, order_ids[None, :], 0), axis=1)[:, None]
    filled = jnp.sum(jnp.where(matches, 1, 0), axis=1).astype(jnp.int32)
    band = jnp.arange(BANDS, dtype=jnp.int32)[None, :]
    parity = block % 2
    k, p, q = tile // 16, (tile // 4) % 4, tile % 4
    reach = parity + k
    apart = reach // 2
    row_first = parity == band
    column_first = reach % 2 == band
    both = row_first & column_first
    neither = ~row_first & ~column_first
    within = jnp.where(both, 0, jnp.where(neither, 2, 3))
    beside = jnp.where(both, 1, jnp.where(column_first, 4, 6 + q // 2))
    across = jnp.where(both, 2, jnp.where(neither, 0, 1))
    place = jnp.where(apart == 0, within, jnp.where(apart == 1, beside, across))
    late = (apart == 1) & ~column_first
    core = jnp.where(late, jnp.where(row_first, 0, 1), q // 2)
    source = band * 16 + p * 4 + (q % 2) * 2 + core + jnp.where(apart == 2, 32, 0)
    return (source * 8 + place).reshape(-1).astype(jnp.int32), filled


def body(spectra, window_count, tile_owner, phases):
    counted = window_count[0]
    windows = spectra.shape[1]
    velocities = phases.shape[2]
    weight = 1.0 / (counted.astype(jnp.float32) * math.sqrt(FB * lax.axis_size("seg")))
    live = (jnp.arange(windows, dtype=jnp.int32) < counted).astype(jnp.float32)
    scale = jnp.concatenate([weight[None], live])
    rows, filled = slot_rows(tile_owner[0], lax.axis_index("blk"), lax.axis_index("seg"))
    bf16, f32 = jnp.bfloat16, jnp.float32
    dma = pltpu.SemaphoreType.DMA
    response = pl.pallas_call(
        kernel,
        out_shape=jax.ShapeDtypeStruct((CAP, BANDS, velocities), f32),
        in_specs=[pl.BlockSpec(memory_space=pltpu.SMEM)] * 3 + [pl.BlockSpec(memory_space=pl.ANY)] * 2,
        out_specs=pl.BlockSpec(memory_space=pltpu.VMEM),
        scratch_shapes=[
            pltpu.VMEM((QUAD, 2, TILE, 2 * PART), bf16),
            pltpu.VMEM((QUAD, TILE, 2 * PART), bf16),
            pltpu.VMEM((10, QUAD, TILE, 2 * PART), bf16),
            pltpu.VMEM((ROUNDS, 4, QUAD, TILE, 2 * TILE), bf16),
            pltpu.VMEM((ROUNDS, 2, QUAD, TILE, 2 * TILE), bf16),
            pltpu.VMEM((ROUNDS, 2, TILE, 2 * TILE), bf16),
            pltpu.VMEM((ROUNDS, 2, 2, TILE, 2 * TILE), bf16),
            pltpu.VMEM((ROUNDS, TILE, 2 * TILE), bf16),
            pltpu.VMEM((ROUNDS, TILE, 2 * TILE), bf16),
            pltpu.VMEM((ROUNDS, TILE, 2 * TILE), f32),
            pltpu.VMEM((TILE, velocities), f32),
            pltpu.VMEM((2 * TILE, 2 * velocities), bf16),
            pltpu.VMEM((16, velocities), f32),
            pltpu.VMEM((64 * 8, velocities), f32),
            dma((QUAD,)),
            dma((1,)),
            dma((2, QUAD)),
            dma((2, 2, QUAD)),
            dma((2, 2, QUAD)),
            dma((2, ROUNDS)),
            dma((2, ROUNDS, 2)),
            dma((2, ROUNDS, 2)),
            dma((2, ROUNDS)),
            dma((32,)),
            dma((32,)),
            dma((32,)),
            dma((32,)),
        ],
        compiler_params=pltpu.CompilerParams(vmem_limit_bytes=60 * 1024 * 1024, has_side_effects=True),
    )(rows, filled, scale, spectra[0], phases)
    return response[None, None]


def solution(mesh):
    placed = (P("seg", None, "blk", None), P("seg"), P("blk", None), P())
    return jax.shard_map(
        body,
        mesh=mesh,
        in_specs=placed,
        out_specs=P("blk", "seg", None, None, None),
        check_vma=False,
    )
```

```python
import math

import jax
import jax.numpy as jnp
from jax import lax
from jax.experimental import pallas as pl
from jax.experimental.pallas import tpu as pltpu
from jax.sharding import PartitionSpec as P

TILE = 128
BANDS = 2
CAP = 8
FB = 512
QUAD = 4
ROUNDS = 10
NEAR_ROUNDS, WHOLE_ROUNDS = 5, 6
PART = 2 * FB
MESH = pl.DeviceIdType.MESH


def pick(index, values):
    total = 0
    for key, value in enumerate(values):
        total = total + jnp.where(index == key, value, 0)
    return total


def kernel(
    place_of, count_ref, spectra_ref, phases_ref, out_ref,
    raw, zs, data, out, core_in, relay_in, ring_in, zhi_in, zhi_out, keep,
    phase, matrix, column, powers, late_powers, turned_powers, near, far, late,
    raw_sem, phase_sem, z_sem, up_sem, dn_sem, core_sem, relay_sem, ring_sem, zhi_sem,
    near_sem, far_sem, late_sem, token, token_up, token_dn,
):
    blk = lax.axis_index("blk")
    seg = lax.axis_index("seg")
    y, zl = blk // 2, blk % 2
    x, zh, core = seg // 4, (seg // 2) % 2, seg % 2
    first, second = zl, 1 - zl
    left, right = (x + 3) % 4, (x + 1) % 4

    def seat(nx, nzh, nc):
        return nx * 4 + nzh * 2 + nc

    z_mate = (2 * y + 1 - zl, seg)
    y_down, y_up = (2 * ((y + 3) % 4) + zl, seg), (2 * ((y + 1) % 4) + zl, seg)
    core_mate, zhi_mate = (blk, seat(x, zh, 1 - core)), (blk, seat(x, 1 - zh, core))
    x_mates = (blk, seat(left, zh, core)), (blk, seat(right, zh, core))
    barrier = pltpu.get_barrier_semaphore()
    for mate in (z_mate, y_down, y_up, core_mate, zhi_mate, *x_mates):
        pl.semaphore_signal(barrier, inc=1, device_id=mate, device_id_type=MESH)

    def remote(src, dst, sems, index, device):
        return pltpu.make_async_remote_copy(
            src_ref=src, dst_ref=dst,
            send_sem=sems.at[(0,) + index], recv_sem=sems.at[(1,) + index],
            device_id=device, device_id_type=MESH,
        )

    def z_copy(j):
        return remote(zs.at[j], data.at[2 * zl, j], z_sem, (j,), z_mate)

    def z_wait(j):
        remote(zs.at[j], data.at[2 * second, j], z_sem, (j,), z_mate).wait_recv()

    def up_copy(p, j):
        return remote(data.at[2 * p, j], data.at[8 + p, j], up_sem, (p, j), y_down)

    def dn_copy(p, j):
        return remote(data.at[2 * p, j], data.at[4 + 2 * p, j], dn_sem, (p, j), y_up)

    def core_copy(n):
        return remote(
            out.at[n, pl.ds(2 * (1 - core), 2)], core_in.at[n], core_sem, (n,), core_mate
        )

    def relay_copy(n, side):
        return remote(
            out.at[n, 2 * core + side, (x + 2) % 4], relay_in.at[n, side], relay_sem, (n, side),
            x_mates[side],
        )

    def ring_copy(n, side):
        to = right if side else left
        return remote(
            out.at[n, pl.ds(2 * core, 2), to], ring_in.at[n, side], ring_sem, (n, side),
            x_mates[side],
        )

    def zhi_copy(n):
        return remote(zhi_out.at[n], zhi_in.at[n], zhi_sem, (n,), zhi_mate)

    def back(i):
        return (i // 16) * 16 + (16 - i % 16) % 16

    def gather_copy(source, target, sems, sent, filed, plane, i):
        device = (2 * ((y + plane) % 4) + (zl + i // 16) % 2, (seg + i % 16) % 16)
        return pltpu.make_async_remote_copy(
            src_ref=source, dst_ref=target.at[filed],
            send_sem=sems.at[0, sent], recv_sem=sems.at[1, filed],
            device_id=device, device_id_type=MESH,
        )

    def near_copy(i, filed):
        return gather_copy(powers.at[pl.ds(0, NEAR_ROUNDS)], near, near_sem, i, filed, 0, i)

    def far_copy(i, filed):
        return gather_copy(powers.at[pl.ds(NEAR_ROUNDS, 1)], far, far_sem, i, filed, 3, i)

    def late_near_copy(i, filed):
        return gather_copy(late_powers, late, late_sem, i, filed, 0, i)

    def late_far_copy(i, filed):
        return gather_copy(late_powers, late, late_sem, i, 32 + filed, 3, i)

    def turned_copy(i, filed):
        return gather_copy(turned_powers, late, late_sem, 32 + i, 64 + filed, 1, i)

    def each(count, action):
        def step(i, carry):
            action(i)
            return carry

        lax.fori_loop(0, count, step, 0)

    def raw_copy(j):
        return pltpu.make_async_copy(
            spectra_ref.at[:, pl.ds(pl.multiple_of(j * TILE, TILE), TILE), :], raw.at[j], raw_sem.at[j]
        )

    phase_copy = pltpu.make_async_copy(phases_ref.at[zl], phase, phase_sem.at[0])
    for j in range(QUAD):
        raw_copy(j).start()
    phase_copy.start()

    count = count_ref[0]
    lives = [jnp.where(w < count, 1.0, 0.0).astype(jnp.float32) for w in range(2)]

    def whiten(j, ahead=False):
        raw_copy(j).wait()

        def some_rows(r):
            rows = pl.ds(pl.multiple_of(r * 16, 16), 16)
            for w in range(2):
                mine = raw[j, w, rows, pl.ds(pl.multiple_of(zl * PART, PART), PART)].astype(jnp.float32)
                theirs = raw[j, w, rows, pl.ds(pl.multiple_of(second * PART, PART), PART)].astype(jnp.float32)
                square = jnp.sum(mine * mine + theirs * theirs, axis=1, keepdims=True)
                scaling = lax.rsqrt(square * (1.0 / (2 * PART)) + 1e-05) * lives[w]
                mine = (mine * scaling).astype(jnp.bfloat16)
                data[2 * zl, j, rows, w * PART : (w + 1) * PART] = mine
                data[2 * zl + 1, j, rows, w * PART : w * PART + FB] = mine[:, FB:]
                data[2 * zl + 1, j, rows, w * PART + FB : (w + 1) * PART] = -mine[:, :FB]
                zs[j, rows, w * PART : (w + 1) * PART] = (theirs * scaling).astype(jnp.bfloat16)

        each(TILE // 16, some_rows)
        if ahead:
            pl.semaphore_wait(barrier, 7)
        z_copy(j).start()
        up_copy(zl, j).start()
        dn_copy(zl, j).start()

    whiten(0, ahead=True)
    each(QUAD - 1, lambda j: whiten(j + 1))

    def flip_to(target, slab, j):
        def some_rows(r):
            rows = pl.ds(pl.multiple_of(r * 16, 16), 16)
            for w in range(2):
                target[rows, w * PART : w * PART + FB] = data[slab, j, rows, w * PART + FB : (w + 1) * PART]
                target[rows, w * PART + FB : (w + 1) * PART] = -data[slab, j, rows, w * PART : w * PART + FB]

        each(TILE // 16, some_rows)

    def flip(slab, j):
        flip_to(data.at[slab + 1, j], slab, j)

    phase_copy.wait()
    angles = phase[...]
    norm_factor = 1.0 / math.sqrt(TILE)
    cosine = (jnp.cos(angles) * norm_factor).astype(jnp.bfloat16)
    sine_part = (jnp.sin(angles) * norm_factor).astype(jnp.bfloat16)
    velocities = angles.shape[1]
    matrix[:TILE, :velocities] = cosine
    matrix[:TILE, velocities:] = sine_part
    matrix[TILE:, :velocities] = -sine_part
    matrix[TILE:, velocities:] = cosine
    total_weight = jnp.full((1, 2 * TILE), count, jnp.int32).astype(jnp.float32)
    total_weight = total_weight * math.sqrt(FB * lax.axis_size("seg"))

    def job(n, h):
        @pl.when(n == 1)
        def _():
            for jj in range(2):
                j = 2 * h + jj
                z_wait(j)
                up_copy(second, j).start()
                dn_copy(second, j).start()
                flip(2 * second, j)
                up_copy(first, j).wait_recv()
                dn_copy(first, j).wait_recv()
                flip(4 + 2 * first, j)

        left_slab = pick(n, [first, first, second, 0, second, 2 + first])
        right_slab = pick(n, [2 * first, 8 + first, 2 * second, 2, 8 + first, 8 + first])
        left_side = data[pl.ds(2 * left_slab, 2)].reshape(2 * QUAD * TILE, 2 * PART)
        right_side = data[right_slab, pl.ds(2 * h, 2)].reshape(2 * TILE, 2 * PART)
        product = multiply(left_side, right_side)
        product = (product / total_weight).astype(jnp.bfloat16).reshape(2, QUAD, TILE, 2 * TILE)
        for jj in range(2):
            columns = slice(jj * TILE, (jj + 1) * TILE)
            out[n, 2 * h + jj, :, :, :TILE] = product[0, :, :, columns]
            out[n, 2 * h + jj, :, :, TILE:] = product[1, :, :, columns]

    def multiply(left_side, right_side):
        return lax.dot_general(
            left_side, right_side, (((1,), (1,)), ((), ())), preferred_element_type=jnp.float32
        )

    def small_job(n, q, r, left_slab, left_chunk, right_slab, right_chunk):
        left_side = data[pl.ds(left_slab, 2), left_chunk].reshape(2 * TILE, 2 * PART)
        product = multiply(left_side, data[right_slab, right_chunk])
        product = (product / total_weight[:, :TILE]).astype(jnp.bfloat16)
        out[n, q, r, :, :TILE] = product[:TILE]
        out[n, q, r, :, TILE:] = product[TILE:]

    def chunk_job(n, j):
        up_copy(second, j).wait_recv()
        flip_to(column, 8 + second, j)
        left_side = jnp.concatenate([data[2 * first], data[2 * second]], axis=0)
        right_side = jnp.concatenate([data[8 + second, j], column[...]], axis=0)
        product = multiply(left_side.reshape(2 * QUAD * TILE, 2 * PART), right_side)
        product = (product / total_weight).reshape(2, QUAD, TILE, 2 * TILE)
        out[n, 0:2, :, :, :TILE] = product[:, :, :, :TILE].astype(jnp.bfloat16)
        out[n, 0:2, :, :, TILE:] = (-product[:, :, :, TILE:]).astype(jnp.bfloat16)
        dn_copy(second, j).wait_recv()
        flip(4 + 2 * second, j)

        def mixed(r):
            small_job(n, 2, r, 6, (1 - zl) * j + zl * r, 8, zl * j + (1 - zl) * r)

        each(QUAD, mixed)
        each(j + 1, lambda r: small_job(n, 3, r, 4 + 2 * second, r, 8 + second, j))

    def add_cores(n):
        core_copy(n).wait_recv()

        def one(t):
            q, r = t // 4, t % 4
            total = out[n, 2 * core + q, r].astype(jnp.float32) + core_in[n, q, r].astype(jnp.float32)
            out[n, 2 * core + q, r] = total.astype(jnp.bfloat16)

        each(8, one)
        for side in range(2):
            relay_copy(n, side).start()

    def add_relayed(n):
        for side in range(2):
            to = right if side else left
            relay_copy(n, side).wait_recv()
            total = out[n, 2 * core + side, to].astype(jnp.float32) + relay_in[n, side].astype(jnp.float32)
            out[n, 2 * core + side, to] = total.astype(jnp.bfloat16)
        for side in range(2):
            ring_copy(n, side).start()

    def add_ring(n):
        for side in range(2):
            ring_copy(n, side).wait_recv()

        def total(z):
            return (
                out[n, 2 * core + z, x].astype(jnp.float32)
                + ring_in[n, 0, z].astype(jnp.float32)
                + ring_in[n, 1, z].astype(jnp.float32)
            )

        zhi_out[n] = total(1 - zh).astype(jnp.bfloat16)
        zhi_copy(n).start()
        keep[n] = total(zh)

    def add_last(n):
        zhi_copy(n).wait_recv()
        stacked = (keep[n] + zhi_in[n].astype(jnp.float32)).astype(jnp.bfloat16)

        def power_of(field):
            squared = field * field
            energy = squared[:, :velocities] + squared[:, velocities:]
            return jnp.sum(energy, axis=0, keepdims=True) * (1.0 / TILE)

        power = power_of(jnp.dot(stacked, matrix[...], preferred_element_type=jnp.float32))
        if isinstance(n, int) and n >= WHOLE_ROUNDS:
            late_powers[n - WHOLE_ROUNDS] = power
            turn = (((0,), (0,)), ((), ()))
            real = lax.dot_general(stacked[:, :TILE], matrix[:TILE], turn, preferred_element_type=jnp.float32)
            imag = lax.dot_general(stacked[:, TILE:], matrix[TILE:], turn, preferred_element_type=jnp.float32)
            turned_powers[n - WHOLE_ROUNDS] = power_of(real - imag)
        else:
            powers[n] = power

    stages = (add_cores, add_relayed, add_ring, add_last)

    def step(n):
        each(2, lambda h: job(n, h))
        core_copy(n).start()
        for behind, stage in enumerate(stages):
            @pl.when(n >= 1 + behind)
            def _():
                stage(n - 1 - behind)

    each(WHOLE_ROUNDS, step)
    pl.semaphore_signal(token, inc=1, device_id=z_mate, device_id_type=MESH)
    steps = [*range(WHOLE_ROUNDS), 6, None, 7, None, 8, None, 9, None, None, None, None]
    for at in range(WHOLE_ROUNDS, len(steps)):
        n = steps[at]
        if n is not None:
            chunk_job(n, n - WHOLE_ROUNDS)
            core_copy(n).start()
        for behind, stage in enumerate(stages):
            before = steps[at - 1 - behind]
            if before is not None:
                stage(before)
        if at == WHOLE_ROUNDS + 1:
            pl.semaphore_wait(token, 1)
            pl.semaphore_signal(token_up, inc=1, device_id=y_up, device_id_type=MESH)
            pl.semaphore_signal(token_dn, inc=1, device_id=y_down, device_id_type=MESH)
        if at == WHOLE_ROUNDS + 3:
            pl.semaphore_wait(token_up, 1)
            pl.semaphore_wait(token_dn, 1)
            near[0] = powers[pl.ds(0, NEAR_ROUNDS)]
            each(31, lambda i: near_copy(i + 1, back(i + 1)).start())
            each(32, lambda i: far_copy(i, back(i)).start())

    late[0] = late_powers[...]
    corner = (core == 1) & (zh == 1)

    @pl.when(core == 0)
    def _():
        each(31, lambda i: late_near_copy(i + 1, back(i + 1)).start())

    @pl.when(core == 1)
    def _():
        each(32, lambda i: late_far_copy(i, back(i)).start())

    @pl.when(corner)
    def _():
        each(32, lambda i: turned_copy(i, back(i)).start())

    each(31, lambda i: near_copy(0, i + 1).wait_recv())
    each(32, lambda i: far_copy(0, i).wait_recv())

    def late_near_wait(k):
        offset = (k // 8) * 16 + core + 2 * (k % 8)

        @pl.when(offset > 0)
        def _():
            late_near_copy(0, offset).wait_recv()

    each(16, late_near_wait)
    each(16, lambda k: late_far_copy(0, (k // 8) * 16 + (1 - core) + 2 * (k % 8)).wait_recv())
    each(8, lambda k: turned_copy(0, (k // 4) * 16 + (3 - seg % 4) + 4 * (k % 4)).wait_recv())

    for c in range(CAP):
        for g in range(BANDS):
            kind, slot, place = [place_of[3 * (c * BANDS + g) + part] for part in range(3)]
            inside = jnp.where(kind == 2, 0, slot)
            row = jnp.where(kind == 0, near[inside, jnp.minimum(place, NEAR_ROUNDS - 1)], far[inside, 0])
            row = jnp.where(kind == 2, late[slot, jnp.minimum(place, QUAD - 1)], row)
            out_ref[0, 0, c, g : g + 1, :] = jnp.where(place_of[3 * CAP * BANDS] > c, row, jnp.zeros_like(row))

    def drain_exchange(j):
        z_copy(j).wait_send()
        for p in range(2):
            up_copy(p, j).wait_send()
            dn_copy(p, j).wait_send()

    each(QUAD, drain_exchange)

    def drain_rounds(n):
        core_copy(n).wait_send()
        for side in range(2):
            relay_copy(n, side).wait_send()
            ring_copy(n, side).wait_send()
        zhi_copy(n).wait_send()

    each(ROUNDS, drain_rounds)
    each(31, lambda i: near_copy(i + 1, 0).wait_send())
    each(32, lambda i: far_copy(i, 0).wait_send())

    @pl.when(core == 0)
    def _():
        each(31, lambda i: late_near_copy(i + 1, 0).wait_send())

    @pl.when(core == 1)
    def _():
        each(32, lambda i: late_far_copy(i, 0).wait_send())

    @pl.when(corner)
    def _():
        each(32, lambda i: turned_copy(i, 0).wait_send())


def find_slots(owner_row, block, seg):
    order_ids = jnp.arange(owner_row.shape[0], dtype=jnp.int32)
    mine = owner_row == seg
    rank_of = jnp.sum(jnp.where(mine[None, :] & (order_ids[None, :] < order_ids[:, None]), 1, 0), axis=1)
    matches = mine[None, :] & (rank_of[None, :] == jnp.arange(CAP, dtype=jnp.int32)[:, None])
    tile = jnp.sum(jnp.where(matches, order_ids[None, :], 0), axis=1)[:, None]
    zl, g = block % 2, jnp.arange(BANDS, dtype=jnp.int32)[None, :]
    k, p, q = tile // 16, (tile // 4) % 4, tile % 4
    reach = zl + k
    apart = reach // 2
    row_first = jnp.where(zl == g, 1, 0)
    column_first = jnp.where(reach % 2 == g, 1, 0)
    firsts = row_first + column_first
    whole = jnp.where(firsts == 2, 0, jnp.where(firsts == 0, 2, 3))
    whole = jnp.where(apart == 1, jnp.where(firsts == 2, 1, 4), whole)
    is_whole = jnp.where(apart == 0, 1, jnp.where(apart == 1, column_first, jnp.where(firsts == 2, 1, 0)))
    turned = jnp.where((apart == 2) & (firsts == 0) & (p > q), 1, 0)
    mixed = jnp.where((apart == 2) & (firsts == 1), 1, 0)
    by_row = jnp.where(mixed == 1, 1 - g, turned)
    chunk = jnp.where(by_row == 1, p, q)
    at_x = jnp.where((1 - is_whole) * by_row == 1, q, p)
    at_zh = jnp.where(is_whole == 1, q % 2, jnp.where(apart == 1, 1 - row_first, 1 - mixed))
    at_core = jnp.where(is_whole == 1, q // 2, jnp.where(apart == 1, 0, 1))
    source = at_x * 4 + at_zh * 2 + at_core
    slot = ((zl + g) % 2) * 16 + (source - seg + 16) % 16
    plane = jnp.where(apart == 2, 1 + turned, 0)
    kind = jnp.where(is_whole == 1, jnp.where(apart == 2, 1, 0), 2)
    slot = jnp.where(is_whole == 1, slot, plane * 32 + slot)
    place = jnp.where(is_whole == 1, jnp.where(apart == 2, 0, whole), chunk)
    places = jnp.stack([jnp.broadcast_to(part, (CAP, BANDS)) for part in (kind, slot, place)], axis=2)
    return jnp.concatenate([places.reshape(-1), jnp.sum(jnp.where(mine, 1, 0))[None]]).astype(jnp.int32)


def body(spectra, window_count, tile_owner, phases):
    velocities = phases.shape[2]
    bf16, f32 = jnp.bfloat16, jnp.float32
    dma = pltpu.SemaphoreType.DMA
    return pl.pallas_call(
        kernel,
        out_shape=jax.ShapeDtypeStruct((1, 1, CAP, BANDS, velocities), f32),
        in_specs=[pl.BlockSpec(memory_space=pltpu.SMEM)] * 2 + [pl.BlockSpec(memory_space=pl.ANY)] * 2,
        out_specs=pl.BlockSpec(memory_space=pltpu.VMEM),
        scratch_shapes=[
            pltpu.VMEM((QUAD, 2, TILE, 2 * PART), bf16),
            pltpu.VMEM((QUAD, TILE, 2 * PART), bf16),
            pltpu.VMEM((10, QUAD, TILE, 2 * PART), bf16),
            pltpu.VMEM((ROUNDS, 4, QUAD, TILE, 2 * TILE), bf16),
            pltpu.VMEM((ROUNDS, 2, QUAD, TILE, 2 * TILE), bf16),
            pltpu.VMEM((ROUNDS, 2, TILE, 2 * TILE), bf16),
            pltpu.VMEM((ROUNDS, 2, 2, TILE, 2 * TILE), bf16),
            pltpu.VMEM((ROUNDS, TILE, 2 * TILE), bf16),
            pltpu.VMEM((ROUNDS, TILE, 2 * TILE), bf16),
            pltpu.VMEM((ROUNDS, TILE, 2 * TILE), f32),
            pltpu.VMEM((TILE, velocities), f32),
            pltpu.VMEM((2 * TILE, 2 * velocities), bf16),
            pltpu.VMEM((TILE, 2 * PART), bf16),
            pltpu.VMEM((WHOLE_ROUNDS, 1, velocities), f32),
            pltpu.VMEM((QUAD, 1, velocities), f32),
            pltpu.VMEM((QUAD, 1, velocities), f32),
            pltpu.VMEM((32, NEAR_ROUNDS, 1, velocities), f32),
            pltpu.VMEM((32, 1, 1, velocities), f32),
            pltpu.VMEM((96, QUAD, 1, velocities), f32),
            dma((QUAD,)),
            dma((1,)),
            dma((2, QUAD)),
            dma((2, 2, QUAD)),
            dma((2, 2, QUAD)),
            dma((2, ROUNDS)),
            dma((2, ROUNDS, 2)),
            dma((2, ROUNDS, 2)),
            dma((2, ROUNDS)),
            dma((2, 32)),
            dma((2, 32)),
            dma((2, 96)),
            pltpu.SemaphoreType.REGULAR,
            pltpu.SemaphoreType.REGULAR,
            pltpu.SemaphoreType.REGULAR,
        ],
        compiler_params=pltpu.CompilerParams(vmem_limit_bytes=60 * 1024 * 1024, has_side_effects=True, collective_id=0),
    )(find_slots(tile_owner[0], lax.axis_index("blk"), lax.axis_index("seg")), window_count, spectra[0], phases)


def solution(mesh):
    placed = (P("seg", None, "blk", None), P("seg"), P("blk", None), P())
    return jax.shard_map(
        body,
        mesh=mesh,
        in_specs=placed,
        out_specs=P("blk", "seg", None, None, None),
        check_vma=False,
    )
```

```python
import math

import jax
import jax.numpy as jnp
from jax import lax
from jax.experimental import pallas as pl
from jax.experimental.pallas import tpu as pltpu
from jax.sharding import PartitionSpec as P

TILE = 128
BANDS = 2
CAP = 8
FB = 512
QUAD = 4
ROUNDS = 10
NEAR_ROUNDS, WHOLE_ROUNDS = 5, 6
SCHEDULE = " ".join((
    "p0 c0 r0 g0",
    "l0 T p1 p2",
    "c1 p3 c2 r1",
    "p4 c3 r2 g1",
    "p5 c4 r3 g2",
    "l1 U p6 c5",
    "r4 g3 l2 p7",
    "c6 r5 g4 l3",
    "c7 r6 g5 l4",
    "p8 r7 g6 l5",
    "c8 g7 l6 p9",
    "r8 c9 E g8",
    "r9 D l7 l8",
    "g9 F l9",
))
PART = 2 * FB
MESH = pl.DeviceIdType.MESH


def pick(index, values):
    total = 0
    for key, value in enumerate(values):
        total = total + jnp.where(index == key, value, 0)
    return total


def kernel(
    place_of, count_ref, spectra_ref, phases_ref, out_ref,
    raw, zs, data, out, core_in, relay_in, ring_in, zhi_in, zhi_out, keep,
    phase, matrix, powers, late_powers, turned_powers, near, far, late,
    raw_sem, phase_sem, z_sem, up_sem, dn_sem, core_sem, relay_sem, ring_sem, zhi_sem,
    near_sem, far_sem, late_sem, token, token_up, token_dn,
):
    blk = lax.axis_index("blk")
    seg = lax.axis_index("seg")
    y, zl = blk // 2, blk % 2
    x, zh, core = seg // 4, (seg // 2) % 2, seg % 2
    first, second = zl, 1 - zl
    left, right = (x + 3) % 4, (x + 1) % 4

    def seat(nx, nzh, nc):
        return nx * 4 + nzh * 2 + nc

    z_mate = (2 * y + 1 - zl, seg)
    y_down, y_up = (2 * ((y + 3) % 4) + zl, seg), (2 * ((y + 1) % 4) + zl, seg)
    core_mate, zhi_mate = (blk, seat(x, zh, 1 - core)), (blk, seat(x, 1 - zh, core))
    x_mates = (blk, seat(left, zh, core)), (blk, seat(right, zh, core))
    barrier = pltpu.get_barrier_semaphore()
    for mate in (z_mate, y_down, y_up, core_mate, zhi_mate, *x_mates):
        pl.semaphore_signal(barrier, inc=1, device_id=mate, device_id_type=MESH)

    def remote(src, dst, sems, index, device):
        return pltpu.make_async_remote_copy(
            src_ref=src, dst_ref=dst,
            send_sem=sems.at[(0,) + index], recv_sem=sems.at[(1,) + index],
            device_id=device, device_id_type=MESH,
        )

    def z_copy(j):
        return remote(zs.at[j], data.at[2 * zl, j], z_sem, (j,), z_mate)

    def z_wait(j):
        remote(zs.at[j], data.at[2 * second, j], z_sem, (j,), z_mate).wait_recv()

    def up_copy(p, j):
        return remote(data.at[2 * p, j], data.at[8 + p, j], up_sem, (p, j), y_down)

    def dn_copy(p, j):
        return remote(data.at[2 * p, j], data.at[4 + 2 * p, j], dn_sem, (p, j), y_up)

    def core_copy(n):
        return remote(
            out.at[n, pl.ds(2 * (1 - core), 2)], core_in.at[n], core_sem, (n,), core_mate
        )

    def relay_copy(n, side):
        return remote(
            out.at[n, 2 * core + side, (x + 2) % 4], relay_in.at[n, side], relay_sem, (n, side),
            x_mates[side],
        )

    def ring_copy(n, side):
        to = right if side else left
        return remote(
            out.at[n, pl.ds(2 * core, 2), to], ring_in.at[n, side], ring_sem, (n, side),
            x_mates[side],
        )

    def zhi_copy(n):
        return remote(zhi_out.at[n], zhi_in.at[n], zhi_sem, (n,), zhi_mate)

    def back(i):
        return (i // 16) * 16 + (16 - i % 16) % 16

    def gather_copy(source, target, sems, sent, filed, plane, i):
        device = (2 * ((y + plane) % 4) + (zl + i // 16) % 2, (seg + i % 16) % 16)
        return pltpu.make_async_remote_copy(
            src_ref=source, dst_ref=target.at[filed],
            send_sem=sems.at[0, sent], recv_sem=sems.at[1, filed],
            device_id=device, device_id_type=MESH,
        )

    def near_copy(i, filed):
        return gather_copy(powers.at[pl.ds(0, NEAR_ROUNDS)], near, near_sem, i, filed, 0, i)

    def far_copy(i, filed):
        return gather_copy(powers.at[pl.ds(NEAR_ROUNDS, 1)], far, far_sem, i, filed, 3, i)

    def late_near_copy(i, filed):
        return gather_copy(late_powers, late, late_sem, i, filed, 0, i)

    def late_far_copy(i, filed):
        return gather_copy(late_powers, late, late_sem, i, 32 + filed, 3, i)

    def turned_copy(i, filed):
        return gather_copy(turned_powers, late, late_sem, 32 + i, 64 + filed, 1, i)

    def each(count, action):
        def step(i, carry):
            action(i)
            return carry

        lax.fori_loop(0, count, step, 0)

    def raw_copy(j):
        return pltpu.make_async_copy(
            spectra_ref.at[:, pl.ds(pl.multiple_of(j * TILE, TILE), TILE), :], raw.at[j], raw_sem.at[j]
        )

    phase_copy = pltpu.make_async_copy(phases_ref.at[zl], phase, phase_sem.at[0])
    for j in range(QUAD):
        raw_copy(j).start()
    phase_copy.start()

    count = count_ref[0]
    lives = [jnp.where(w < count, 1.0, 0.0).astype(jnp.float32) for w in range(2)]

    def whiten(j, ahead=False):
        raw_copy(j).wait()

        def some_rows(r):
            rows = pl.ds(pl.multiple_of(r * 16, 16), 16)
            for w in range(2):
                mine = raw[j, w, rows, pl.ds(pl.multiple_of(zl * PART, PART), PART)].astype(jnp.float32)
                theirs = raw[j, w, rows, pl.ds(pl.multiple_of(second * PART, PART), PART)].astype(jnp.float32)
                square = jnp.sum(mine * mine + theirs * theirs, axis=1, keepdims=True)
                scaling = lax.rsqrt(square * (1.0 / (2 * PART)) + 1e-05) * lives[w]
                mine = (mine * scaling).astype(jnp.bfloat16)
                data[2 * zl, j, rows, w * PART : (w + 1) * PART] = mine
                data[2 * zl + 1, j, rows, w * PART : w * PART + FB] = mine[:, FB:]
                data[2 * zl + 1, j, rows, w * PART + FB : (w + 1) * PART] = -mine[:, :FB]
                zs[j, rows, w * PART : (w + 1) * PART] = (theirs * scaling).astype(jnp.bfloat16)

        each(TILE // 16, some_rows)
        if ahead:
            pl.semaphore_wait(barrier, 7)
        z_copy(j).start()
        up_copy(zl, j).start()
        dn_copy(zl, j).start()

    whiten(0, ahead=True)
    each(QUAD - 1, lambda j: whiten(j + 1))

    def flip_to(target, slab, j):
        def some_rows(r):
            rows = pl.ds(pl.multiple_of(r * 16, 16), 16)
            for w in range(2):
                target[rows, w * PART : w * PART + FB] = data[slab, j, rows, w * PART + FB : (w + 1) * PART]
                target[rows, w * PART + FB : (w + 1) * PART] = -data[slab, j, rows, w * PART : w * PART + FB]

        each(TILE // 16, some_rows)

    def flip(slab, j):
        flip_to(data.at[slab + 1, j], slab, j)

    phase_copy.wait()
    angles = phase[...]
    norm_factor = 1.0 / math.sqrt(TILE)
    cosine = (jnp.cos(angles) * norm_factor).astype(jnp.bfloat16)
    sine_part = (jnp.sin(angles) * norm_factor).astype(jnp.bfloat16)
    velocities = angles.shape[1]
    matrix[:TILE, :velocities] = cosine
    matrix[:TILE, velocities:] = sine_part
    matrix[TILE:, :velocities] = -sine_part
    matrix[TILE:, velocities:] = cosine
    total_weight = jnp.full((1, 2 * TILE), count, jnp.int32).astype(jnp.float32)
    weight = 1.0 / (total_weight * math.sqrt(FB * lax.axis_size("seg")))

    def job(n, h):
        @pl.when(n == 1)
        def _():
            for jj in range(2):
                j = 2 * h + jj
                z_wait(j)
                up_copy(second, j).start()
                dn_copy(second, j).start()
                flip(2 * second, j)
                up_copy(first, j).wait_recv()
                dn_copy(first, j).wait_recv()
                flip(4 + 2 * first, j)

        left_slab = pick(n, [first, first, second, 0, second, 2 + first])
        right_slab = pick(n, [2 * first, 8 + first, 2 * second, 2, 8 + first, 8 + first])
        left_side = data[pl.ds(2 * left_slab, 2)].reshape(2 * QUAD * TILE, 2 * PART)
        right_side = data[right_slab, pl.ds(2 * h, 2)].reshape(2 * TILE, 2 * PART)
        product = multiply(left_side, right_side)
        product = (product * weight).astype(jnp.bfloat16).reshape(2, QUAD, TILE, 2 * TILE)
        for jj in range(2):
            columns = slice(jj * TILE, (jj + 1) * TILE)
            out[n, 2 * h + jj, :, :, :TILE] = product[0, :, :, columns]
            out[n, 2 * h + jj, :, :, TILE:] = product[1, :, :, columns]

    def multiply(left_side, right_side):
        return lax.dot_general(
            left_side, right_side, (((1,), (1,)), ((), ())), preferred_element_type=jnp.float32
        )

    def store(n, q, left_side, right_side):
        count_rows = left_side.shape[0]
        product = multiply(left_side.reshape(count_rows * TILE, 2 * PART), right_side) * weight
        product = product.reshape(count_rows, TILE, 2 * TILE)
        for r in range(0, count_rows, QUAD):
            rows = slice(r, min(r + QUAD, count_rows))
            out[n, q + r // QUAD, : rows.stop - r, :, :TILE] = product[rows, :, :TILE].astype(jnp.bfloat16)
            out[n, q + r // QUAD, : rows.stop - r, :, TILE:] = (-product[rows, :, TILE:]).astype(jnp.bfloat16)

    def chunk_job(n, j):
        up_copy(second, j).wait_recv()
        flip_to(data.at[10, j], 8 + second, j)
        chunk = jnp.concatenate([data[8 + second, j], data[10, j]], axis=0)
        store(n, 0, jnp.concatenate([data[2 * first], data[2 * second]], axis=0), chunk)
        dn_copy(second, j).wait_recv()
        flip(4 + 2 * second, j)
        store(n, 3, data[4 + 2 * second, 0 : j + 1], chunk)
        store(n, 2, data[8 - 2 * zl], jnp.concatenate([data[6 + 2 * zl, j], data[7 + 3 * zl, j]], axis=0))

    def add_cores(n):
        core_copy(n).wait_recv()

        def one(t):
            q, r = t // 4, t % 4
            out[n, 2 * core + q, r] = out[n, 2 * core + q, r] + core_in[n, q, r]

        each(8, one)
        for side in range(2):
            relay_copy(n, side).start()

    def add_relayed(n):
        for side in range(2):
            to = right if side else left
            relay_copy(n, side).wait_recv()
            out[n, 2 * core + side, to] = out[n, 2 * core + side, to] + relay_in[n, side]
        for side in range(2):
            ring_copy(n, side).start()

    def add_ring(n):
        for side in range(2):
            ring_copy(n, side).wait_recv()

        def total(z):
            return (
                out[n, 2 * core + z, x].astype(jnp.float32)
                + ring_in[n, 0, z].astype(jnp.float32)
                + ring_in[n, 1, z].astype(jnp.float32)
            )

        zhi_out[n] = total(1 - zh).astype(jnp.bfloat16)
        zhi_copy(n).start()
        keep[n] = total(zh)

    def add_last(n):
        zhi_copy(n).wait_recv()
        stacked = (keep[n] + zhi_in[n].astype(jnp.float32)).astype(jnp.bfloat16)

        def power_of(field):
            squared = field * field
            energy = squared[:, :velocities] + squared[:, velocities:]
            return jnp.sum(energy, axis=0, keepdims=True) * (1.0 / TILE)

        power = power_of(jnp.dot(stacked, matrix[...], preferred_element_type=jnp.float32))
        if n >= WHOLE_ROUNDS:
            turn = (((0,), (0,)), ((), ()))
            real = lax.dot_general(stacked[:, :TILE], matrix[:TILE], turn, preferred_element_type=jnp.float32)
            imag = lax.dot_general(stacked[:, TILE:], matrix[TILE:], turn, preferred_element_type=jnp.float32)
            turned = power_of(real - imag)
            turned_powers[n - WHOLE_ROUNDS] = turned
            mirrored = (zl == 0) & (core == 1) & (zh == 0)
            late_powers[n - WHOLE_ROUNDS] = jnp.where(mirrored, turned, power)
        else:
            powers[n] = power

    def drain_exchange(j):
        z_copy(j).wait_send()
        for p in range(2):
            up_copy(p, j).wait_send()
            dn_copy(p, j).wait_send()


    def drain_rounds(n):
        core_copy(n).wait_send()
        for side in range(2):
            relay_copy(n, side).wait_send()
            ring_copy(n, side).wait_send()
        zhi_copy(n).wait_send()

    def products(n):
        if n < WHOLE_ROUNDS:
            each(2, lambda h: job(n, h))
        else:
            chunk_job(n, n - WHOLE_ROUNDS)
        core_copy(n).start()

    def send_early():
        pl.semaphore_wait(token_up, 1)
        pl.semaphore_wait(token_dn, 1)
        near[0] = powers[pl.ds(0, NEAR_ROUNDS)]
        each(31, lambda i: near_copy(i + 1, back(i + 1)).start())
        each(32, lambda i: far_copy(i, back(i)).start())

    def drain_early():
        each(31, lambda i: near_copy(0, i + 1).wait_recv())
        each(32, lambda i: far_copy(0, i).wait_recv())
        each(31, lambda i: near_copy(i + 1, 0).wait_send())
        each(32, lambda i: far_copy(i, 0).wait_send())

    def drain_first():
        each(QUAD, drain_exchange)
        each(ROUNDS - 2, drain_rounds)

    def tell_pair():
        pl.semaphore_signal(token, inc=1, device_id=z_mate, device_id_type=MESH)

    def tell_planes():
        pl.semaphore_wait(token, 1)
        pl.semaphore_signal(token_up, inc=1, device_id=y_up, device_id_type=MESH)
        pl.semaphore_signal(token_dn, inc=1, device_id=y_down, device_id_type=MESH)

    acts = dict(p=products, c=add_cores, r=add_relayed, g=add_ring, l=add_last)
    others = dict(T=tell_pair, U=tell_planes, E=send_early, D=drain_first, F=drain_early)
    for event in SCHEDULE.split():
        if event in others:
            others[event]()
        else:
            acts[event[0]](int(event[1]))

    late[0] = late_powers[...]
    corner = (core == 1) & (zh == 1)

    @pl.when(core == 0)
    def _():
        each(31, lambda i: late_near_copy(i + 1, back(i + 1)).start())

    @pl.when(core == 1)
    def _():
        each(32, lambda i: late_far_copy(i, back(i)).start())

    @pl.when(corner)
    def _():
        each(32, lambda i: turned_copy(i, back(i)).start())

    def late_near_wait(k):
        offset = (k // 8) * 16 + core + 2 * (k % 8)

        @pl.when(offset > 0)
        def _():
            late_near_copy(0, offset).wait_recv()

    each(16, late_near_wait)
    each(16, lambda k: late_far_copy(0, (k // 8) * 16 + (1 - core) + 2 * (k % 8)).wait_recv())
    each(8, lambda k: turned_copy(0, (k // 4) * 16 + (3 - seg % 4) + 4 * (k % 4)).wait_recv())

    for c in range(CAP):
        for g in range(BANDS):
            kind, slot, place = [place_of[c, part * BANDS + g] for part in range(3)]
            inside = jnp.where(kind < 2, slot, 0)
            row = jnp.where(kind == 0, near[inside, jnp.minimum(place, NEAR_ROUNDS - 1)], far[inside, 0])
            row = jnp.where(kind == 2, late[slot, jnp.minimum(place, QUAD - 1)], row)
            out_ref[0, 0, c, g : g + 1, :] = jnp.where(kind < 3, row, jnp.zeros_like(row))

    each(2, lambda n: drain_rounds(ROUNDS - 2 + n))

    @pl.when(core == 0)
    def _():
        each(31, lambda i: late_near_copy(i + 1, 0).wait_send())

    @pl.when(core == 1)
    def _():
        each(32, lambda i: late_far_copy(i, 0).wait_send())

    @pl.when(corner)
    def _():
        each(32, lambda i: turned_copy(i, 0).wait_send())


def find_slots(owner_row, block, seg):
    order_ids = jnp.arange(owner_row.shape[0], dtype=jnp.int32)
    mine = owner_row == seg
    rank_of = jnp.sum(jnp.where(mine[None, :] & (order_ids[None, :] < order_ids[:, None]), 1, 0), axis=1)
    matches = mine[None, :] & (rank_of[None, :] == jnp.arange(CAP, dtype=jnp.int32)[:, None])
    tile = jnp.sum(jnp.where(matches, order_ids[None, :], 0), axis=1)[:, None]
    zl, g = block % 2, jnp.arange(BANDS, dtype=jnp.int32)[None, :]
    k, p, q = tile // 16, (tile // 4) % 4, tile % 4
    reach = zl + k
    apart = reach // 2
    row_first = jnp.where(zl == g, 1, 0)
    column_first = jnp.where(reach % 2 == g, 1, 0)
    firsts = row_first + column_first
    whole = jnp.where(firsts == 2, 0, jnp.where(firsts == 0, 2, 3))
    whole = jnp.where(apart == 1, jnp.where(firsts == 2, 1, 4), whole)
    is_whole = jnp.where(apart == 0, 1, jnp.where(apart == 1, column_first, jnp.where(firsts == 2, 1, 0)))
    turned = jnp.where((apart == 2) & (firsts == 0) & (p > q), 1, 0)
    mixed = jnp.where((apart == 2) & (firsts == 1), 1, 0)
    by_row = jnp.where(mixed == 1, 1 - g, turned)
    chunk = jnp.where(by_row == 1, p, q)
    at_x = jnp.where((1 - is_whole) * by_row == 1, q, p)
    at_zh = jnp.where(is_whole == 1, q % 2, jnp.where(apart == 1, 1 - row_first, 1 - mixed))
    at_core = jnp.where(is_whole == 1, q // 2, jnp.where(apart == 1, 0, 1))
    source = at_x * 4 + at_zh * 2 + at_core
    slot = ((zl + g) % 2) * 16 + (source - seg + 16) % 16
    plane = jnp.where(apart == 2, 1 + turned, 0)
    kind = jnp.where(is_whole == 1, jnp.where(apart == 2, 1, 0), 2)
    kind = jnp.where(jnp.sum(jnp.where(matches, 1, 0), axis=1)[:, None] == 1, kind, 3)
    slot = jnp.where(is_whole == 1, slot, plane * 32 + slot)
    place = jnp.where(is_whole == 1, jnp.where(apart == 2, 0, whole), chunk)
    parts = [jnp.broadcast_to(part, (CAP, BANDS)) for part in (kind, slot, place)]
    return jnp.concatenate(parts, axis=1).astype(jnp.int32)


def body(spectra, window_count, tile_owner, phases):
    velocities = phases.shape[2]
    bf16, f32 = jnp.bfloat16, jnp.float32
    dma = pltpu.SemaphoreType.DMA
    return pl.pallas_call(
        kernel,
        out_shape=jax.ShapeDtypeStruct((1, 1, CAP, BANDS, velocities), f32),
        in_specs=[pl.BlockSpec(memory_space=pltpu.SMEM)] * 2 + [pl.BlockSpec(memory_space=pl.ANY)] * 2,
        out_specs=pl.BlockSpec(memory_space=pltpu.VMEM),
        scratch_shapes=[
            pltpu.VMEM((QUAD, 2, TILE, 2 * PART), bf16),
            pltpu.VMEM((QUAD, TILE, 2 * PART), bf16),
            pltpu.VMEM((11, QUAD, TILE, 2 * PART), bf16),
            pltpu.VMEM((ROUNDS, 4, QUAD, TILE, 2 * TILE), bf16),
            pltpu.VMEM((ROUNDS, 2, QUAD, TILE, 2 * TILE), bf16),
            pltpu.VMEM((ROUNDS, 2, TILE, 2 * TILE), bf16),
            pltpu.VMEM((ROUNDS, 2, 2, TILE, 2 * TILE), bf16),
            pltpu.VMEM((ROUNDS, TILE, 2 * TILE), bf16),
            pltpu.VMEM((ROUNDS, TILE, 2 * TILE), bf16),
            pltpu.VMEM((ROUNDS, TILE, 2 * TILE), f32),
            pltpu.VMEM((TILE, velocities), f32),
            pltpu.VMEM((2 * TILE, 2 * velocities), bf16),
            pltpu.VMEM((WHOLE_ROUNDS, 1, velocities), f32),
            pltpu.VMEM((QUAD, 1, velocities), f32),
            pltpu.VMEM((QUAD, 1, velocities), f32),
            pltpu.VMEM((32, NEAR_ROUNDS, 1, velocities), f32),
            pltpu.VMEM((32, 1, 1, velocities), f32),
            pltpu.VMEM((96, QUAD, 1, velocities), f32),
            dma((QUAD,)),
            dma((1,)),
            dma((2, QUAD)),
            dma((2, 2, QUAD)),
            dma((2, 2, QUAD)),
            dma((2, ROUNDS)),
            dma((2, ROUNDS, 2)),
            dma((2, ROUNDS, 2)),
            dma((2, ROUNDS)),
            dma((2, 32)),
            dma((2, 32)),
            dma((2, 96)),
            pltpu.SemaphoreType.REGULAR,
            pltpu.SemaphoreType.REGULAR,
            pltpu.SemaphoreType.REGULAR,
        ],
        compiler_params=pltpu.CompilerParams(vmem_limit_bytes=60 * 1024 * 1024, has_side_effects=True, collective_id=0),
    )(find_slots(tile_owner[0], lax.axis_index("blk"), lax.axis_index("seg")), window_count, spectra[0], phases)


def solution(mesh):
    placed = (P("seg", None, "blk", None), P("seg"), P("blk", None), P())
    return jax.shard_map(
        body,
        mesh=mesh,
        in_specs=placed,
        out_specs=P("blk", "seg", None, None, None),
        check_vma=False,
    )
```

```python
import math

import jax
import jax.numpy as jnp
from jax import lax
from jax.experimental import pallas as pl
from jax.experimental.pallas import tpu as pltpu
from jax.sharding import PartitionSpec as P

TILE = 128
BANDS = 2
CAP = 8
FB = 512
QUAD = 4
ROUNDS = 10
NEAR_ROUNDS, WHOLE_ROUNDS = 5, 6
SCHEDULE = " ".join((
    "p0 c0 r0 g0",
    "l0 T p1 p2",
    "c1 p3 c2 r1",
    "p4 c3 r2 g1",
    "p5 c4 r3 g2",
    "l1 U p6 c5",
    "r4 g3 l2 p7",
    "c6 r5 g4 l3",
    "c7 r6 g5 l4",
    "p8 r7 g6 l5",
    "c8 g7 l6 p9",
    "r8 c9 E g8",
    "r9 D l7 l8",
    "g9 F l9",
))
PART = 2 * FB
MESH = pl.DeviceIdType.MESH


def pick(index, values):
    total = 0
    for key, value in enumerate(values):
        total = total + jnp.where(index == key, value, 0)
    return total


def kernel(
    place_of, count_ref, spectra_ref, phases_ref, out_ref,
    raw, zs, data, out, core_in, relay_in, ring_in, zhi_in, zhi_out, keep,
    phase, matrix, powers, late_powers, turned_powers, near, far, late,
    raw_sem, phase_sem, z_sem, up_sem, dn_sem, core_sem, relay_sem, ring_sem, zhi_sem,
    near_sem, far_sem, late_sem, token, token_up, token_dn,
):
    blk = lax.axis_index("blk")
    seg = lax.axis_index("seg")
    y, zl = blk // 2, blk % 2
    x, zh, core = seg // 4, (seg // 2) % 2, seg % 2
    first, second = zl, 1 - zl
    left, right = (x + 3) % 4, (x + 1) % 4

    def seat(nx, nzh, nc):
        return nx * 4 + nzh * 2 + nc

    z_mate = (2 * y + 1 - zl, seg)
    y_down, y_up = (2 * ((y + 3) % 4) + zl, seg), (2 * ((y + 1) % 4) + zl, seg)
    core_mate, zhi_mate = (blk, seat(x, zh, 1 - core)), (blk, seat(x, 1 - zh, core))
    x_mates = (blk, seat(left, zh, core)), (blk, seat(right, zh, core))
    barrier = pltpu.get_barrier_semaphore()
    for mate in (z_mate, y_down, y_up, core_mate, zhi_mate, *x_mates):
        pl.semaphore_signal(barrier, inc=1, device_id=mate, device_id_type=MESH)

    def remote(src, dst, sems, index, device):
        return pltpu.make_async_remote_copy(
            src_ref=src, dst_ref=dst,
            send_sem=sems.at[(0,) + index], recv_sem=sems.at[(1,) + index],
            device_id=device, device_id_type=MESH,
        )

    def z_copy(j):
        return remote(zs.at[j], data.at[2 * zl, j], z_sem, (j,), z_mate)

    def z_wait(j):
        remote(zs.at[j], data.at[2 * second, j], z_sem, (j,), z_mate).wait_recv()

    def up_copy(p, j):
        return remote(data.at[2 * p, j], data.at[8 + p, j], up_sem, (p, j), y_down)

    def dn_copy(p, j):
        return remote(data.at[2 * p, j], data.at[4 + 2 * p, j], dn_sem, (p, j), y_up)

    def core_copy(n):
        return remote(
            out.at[n, pl.ds(2 * (1 - core), 2)], core_in.at[n], core_sem, (n,), core_mate
        )

    def relay_copy(n, side):
        return remote(
            out.at[n, 2 * core + side, (x + 2) % 4], relay_in.at[n, side], relay_sem, (n, side),
            x_mates[side],
        )

    def ring_copy(n, side):
        to = right if side else left
        return remote(
            out.at[n, pl.ds(2 * core, 2), to], ring_in.at[n, side], ring_sem, (n, side),
            x_mates[side],
        )

    def zhi_copy(n):
        return remote(zhi_out.at[n], zhi_in.at[n], zhi_sem, (n,), zhi_mate)

    def back(i):
        return (i // 16) * 16 + (16 - i % 16) % 16

    def gather_copy(source, target, sems, sent, filed, plane, i):
        device = (2 * ((y + plane) % 4) + (zl + i // 16) % 2, (seg + i % 16) % 16)
        return pltpu.make_async_remote_copy(
            src_ref=source, dst_ref=target.at[filed],
            send_sem=sems.at[0, sent], recv_sem=sems.at[1, filed],
            device_id=device, device_id_type=MESH,
        )

    def near_copy(i, filed):
        return gather_copy(powers.at[pl.ds(0, NEAR_ROUNDS)], near, near_sem, i, filed, 0, i)

    def far_copy(i, filed):
        return gather_copy(powers.at[pl.ds(NEAR_ROUNDS, 1)], far, far_sem, i, filed, 3, i)

    def late_near_copy(i, filed):
        return gather_copy(late_powers, late, late_sem, i, filed, 0, i)

    def late_far_copy(i, filed):
        return gather_copy(late_powers, late, late_sem, i, 32 + filed, 3, i)

    def turned_copy(i, filed):
        return gather_copy(turned_powers, late, late_sem, 32 + i, 64 + filed, 1, i)

    def each(count, action):
        def step(i, carry):
            action(i)
            return carry

        lax.fori_loop(0, count, step, 0)

    def raw_copy(j):
        return pltpu.make_async_copy(
            spectra_ref.at[:, pl.ds(pl.multiple_of(j * TILE, TILE), TILE), :], raw.at[j], raw_sem.at[j]
        )

    phase_copy = pltpu.make_async_copy(phases_ref.at[zl], phase, phase_sem.at[0])
    for j in range(QUAD):
        raw_copy(j).start()
    phase_copy.start()

    count = count_ref[0]
    lives = [jnp.where(w < count, 1.0, 0.0).astype(jnp.float32) for w in range(2)]

    def whiten(j, ahead=False):
        raw_copy(j).wait()

        def some_rows(r):
            rows = pl.ds(pl.multiple_of(r * 16, 16), 16)
            for w in range(2):
                mine = raw[j, w, rows, pl.ds(pl.multiple_of(zl * PART, PART), PART)].astype(jnp.float32)
                theirs = raw[j, w, rows, pl.ds(pl.multiple_of(second * PART, PART), PART)].astype(jnp.float32)
                square = jnp.sum(mine * mine + theirs * theirs, axis=1, keepdims=True)
                scaling = lax.rsqrt(square * (1.0 / (2 * PART)) + 1e-05) * lives[w]
                mine = (mine * scaling).astype(jnp.bfloat16)
                data[2 * zl, j, rows, w * PART : (w + 1) * PART] = mine
                data[2 * zl + 1, j, rows, w * PART : w * PART + FB] = mine[:, FB:]
                data[2 * zl + 1, j, rows, w * PART + FB : (w + 1) * PART] = -mine[:, :FB]
                zs[j, rows, w * PART : (w + 1) * PART] = (theirs * scaling).astype(jnp.bfloat16)

        each(TILE // 16, some_rows)
        if ahead:
            pl.semaphore_wait(barrier, 7)
        z_copy(j).start()
        up_copy(zl, j).start()
        dn_copy(zl, j).start()

    whiten(0, ahead=True)
    each(QUAD - 1, lambda j: whiten(j + 1))

    def flip_to(target, slab, j):
        def some_rows(r):
            rows = pl.ds(pl.multiple_of(r * 16, 16), 16)
            for w in range(2):
                target[rows, w * PART : w * PART + FB] = data[slab, j, rows, w * PART + FB : (w + 1) * PART]
                target[rows, w * PART + FB : (w + 1) * PART] = -data[slab, j, rows, w * PART : w * PART + FB]

        each(TILE // 16, some_rows)

    def flip(slab, j):
        flip_to(data.at[slab + 1, j], slab, j)

    phase_copy.wait()
    angles = phase[...]
    norm_factor = 1.0 / math.sqrt(TILE)
    cosine = (jnp.cos(angles) * norm_factor).astype(jnp.bfloat16)
    sine_part = (jnp.sin(angles) * norm_factor).astype(jnp.bfloat16)
    velocities = angles.shape[1]
    matrix[:TILE, :velocities] = cosine
    matrix[:TILE, velocities:] = sine_part
    matrix[TILE:, :velocities] = -sine_part
    matrix[TILE:, velocities:] = cosine
    total_weight = jnp.full((1, 2 * TILE), count, jnp.int32).astype(jnp.float32)
    weight = 1.0 / (total_weight * math.sqrt(FB * lax.axis_size("seg")))

    def job(n, h):
        @pl.when(n == 1)
        def _():
            for jj in range(2):
                j = 2 * h + jj
                z_wait(j)
                up_copy(second, j).start()
                dn_copy(second, j).start()
                flip(2 * second, j)
                up_copy(first, j).wait_recv()
                dn_copy(first, j).wait_recv()
                flip(4 + 2 * first, j)

        left_slab = pick(n, [first, first, second, 0, second, 2 + first])
        right_slab = pick(n, [2 * first, 8 + first, 2 * second, 2, 8 + first, 8 + first])
        left_side = data[pl.ds(2 * left_slab, 2)].reshape(2 * QUAD * TILE, 2 * PART)
        right_side = data[right_slab, pl.ds(2 * h, 2)].reshape(2 * TILE, 2 * PART)
        product = multiply(left_side, right_side)
        product = (product * weight).astype(jnp.bfloat16).reshape(2, QUAD, TILE, 2 * TILE)
        for jj in range(2):
            columns = slice(jj * TILE, (jj + 1) * TILE)
            out[n, 2 * h + jj, :, :, :TILE] = product[0, :, :, columns]
            out[n, 2 * h + jj, :, :, TILE:] = product[1, :, :, columns]

    def multiply(left_side, right_side):
        return lax.dot_general(
            left_side, right_side, (((1,), (1,)), ((), ())), preferred_element_type=jnp.float32
        )

    def store(n, q, left_side, right_side):
        count_rows = left_side.shape[0]
        product = multiply(left_side.reshape(count_rows * TILE, 2 * PART), right_side) * weight
        product = product.reshape(count_rows, TILE, 2 * TILE)
        for r in range(0, count_rows, QUAD):
            rows = slice(r, min(r + QUAD, count_rows))
            out[n, q + r // QUAD, : rows.stop - r, :, :TILE] = product[rows, :, :TILE].astype(jnp.bfloat16)
            out[n, q + r // QUAD, : rows.stop - r, :, TILE:] = (-product[rows, :, TILE:]).astype(jnp.bfloat16)

    def chunk_job(n, j):
        up_copy(second, j).wait_recv()
        flip_to(data.at[10, j], 8 + second, j)
        chunk = jnp.concatenate([data[8 + second, j], data[10, j]], axis=0)
        store(n, 0, jnp.concatenate([data[2 * first], data[2 * second]], axis=0), chunk)
        dn_copy(second, j).wait_recv()
        flip(4 + 2 * second, j)
        store(n, 3, data[4 + 2 * second, 0 : j + 1], chunk)
        store(n, 2, data[8 - 2 * zl], jnp.concatenate([data[6 + 2 * zl, j], data[7 + 3 * zl, j]], axis=0))

    def add_cores(n):
        core_copy(n).wait_recv()

        def one(t):
            q, r = t // 4, t % 4
            out[n, 2 * core + q, r] = out[n, 2 * core + q, r] + core_in[n, q, r]

        each(8, one)
        for side in range(2):
            relay_copy(n, side).start()

    def add_relayed(n):
        for side in range(2):
            to = right if side else left
            relay_copy(n, side).wait_recv()
            out[n, 2 * core + side, to] = out[n, 2 * core + side, to] + relay_in[n, side]
        for side in range(2):
            ring_copy(n, side).start()

    def add_ring(n):
        for side in range(2):
            ring_copy(n, side).wait_recv()

        def total(z):
            return (
                out[n, 2 * core + z, x].astype(jnp.float32)
                + ring_in[n, 0, z].astype(jnp.float32)
                + ring_in[n, 1, z].astype(jnp.float32)
            )

        zhi_out[n] = total(1 - zh).astype(jnp.bfloat16)
        zhi_copy(n).start()
        keep[n] = total(zh)

    def add_last(n):
        zhi_copy(n).wait_recv()
        stacked = (keep[n] + zhi_in[n].astype(jnp.float32)).astype(jnp.bfloat16)

        def power_of(field):
            squared = field * field
            energy = squared[:, :velocities] + squared[:, velocities:]
            return jnp.sum(energy, axis=0, keepdims=True) * (1.0 / TILE)

        power = power_of(jnp.dot(stacked, matrix[...], preferred_element_type=jnp.float32))
        if n >= WHOLE_ROUNDS:
            turn = (((0,), (0,)), ((), ()))
            real = lax.dot_general(stacked[:, :TILE], matrix[:TILE], turn, preferred_element_type=jnp.float32)
            imag = lax.dot_general(stacked[:, TILE:], matrix[TILE:], turn, preferred_element_type=jnp.float32)
            turned = power_of(real - imag)
            turned_powers[n - WHOLE_ROUNDS] = turned
            mirrored = (zl == 0) & (core == 1) & (zh == 0)
            late_powers[n - WHOLE_ROUNDS] = jnp.where(mirrored, turned, power)
        else:
            powers[n] = power

    def drain_exchange(j):
        z_copy(j).wait_send()
        for p in range(2):
            up_copy(p, j).wait_send()
            dn_copy(p, j).wait_send()


    def drain_rounds(n):
        core_copy(n).wait_send()
        for side in range(2):
            relay_copy(n, side).wait_send()
            ring_copy(n, side).wait_send()
        zhi_copy(n).wait_send()

    def products(n):
        if n < WHOLE_ROUNDS:
            each(2, lambda h: job(n, h))
        else:
            chunk_job(n, n - WHOLE_ROUNDS)
        core_copy(n).start()

    def send_early():
        pl.semaphore_wait(token_up, 1)
        pl.semaphore_wait(token_dn, 1)
        near[0] = powers[pl.ds(0, NEAR_ROUNDS)]
        each(31, lambda i: near_copy(i + 1, back(i + 1)).start())
        each(32, lambda i: far_copy(i, back(i)).start())

    def drain_early():
        each(31, lambda i: near_copy(0, i + 1).wait_recv())
        each(32, lambda i: far_copy(0, i).wait_recv())
        each(31, lambda i: near_copy(i + 1, 0).wait_send())
        each(32, lambda i: far_copy(i, 0).wait_send())

    def drain_first():
        each(QUAD, drain_exchange)
        each(ROUNDS - 2, drain_rounds)

    def tell_pair():
        pl.semaphore_signal(token, inc=1, device_id=z_mate, device_id_type=MESH)

    def tell_planes():
        pl.semaphore_wait(token, 1)
        pl.semaphore_signal(token_up, inc=1, device_id=y_up, device_id_type=MESH)
        pl.semaphore_signal(token_dn, inc=1, device_id=y_down, device_id_type=MESH)

    acts = dict(p=products, c=add_cores, r=add_relayed, g=add_ring, l=add_last)
    others = dict(T=tell_pair, U=tell_planes, E=send_early, D=drain_first, F=drain_early)
    for event in SCHEDULE.split():
        if event in others:
            others[event]()
        else:
            acts[event[0]](int(event[1]))

    late[0] = late_powers[...]
    corner = (core == 1) & (zh == 1)

    @pl.when(core == 0)
    def _():
        each(31, lambda i: late_near_copy(i + 1, back(i + 1)).start())

    @pl.when(core == 1)
    def _():
        each(32, lambda i: late_far_copy(i, back(i)).start())

    @pl.when(corner)
    def _():
        each(32, lambda i: turned_copy(i, back(i)).start())

    def late_near_wait(k):
        offset = (k // 8) * 16 + core + 2 * (k % 8)

        @pl.when(offset > 0)
        def _():
            late_near_copy(0, offset).wait_recv()

    each(16, late_near_wait)
    each(16, lambda k: late_far_copy(0, (k // 8) * 16 + (1 - core) + 2 * (k % 8)).wait_recv())
    each(8, lambda k: turned_copy(0, (k // 4) * 16 + (3 - seg % 4) + 4 * (k % 4)).wait_recv())

    for c in range(CAP):
        for g in range(BANDS):
            kind, slot, place = [place_of[c, part * BANDS + g] for part in range(3)]
            inside = jnp.where(kind < 2, slot, 0)
            row = jnp.where(kind == 0, near[inside, jnp.minimum(place, NEAR_ROUNDS - 1)], far[inside, 0])
            row = jnp.where(kind == 2, late[slot, jnp.minimum(place, QUAD - 1)], row)
            out_ref[0, 0, c, g : g + 1, :] = jnp.where(kind < 3, row, jnp.zeros_like(row))

    each(2, lambda n: drain_rounds(ROUNDS - 2 + n))

    @pl.when(core == 0)
    def _():
        each(31, lambda i: late_near_copy(i + 1, 0).wait_send())

    @pl.when(core == 1)
    def _():
        each(32, lambda i: late_far_copy(i, 0).wait_send())

    @pl.when(corner)
    def _():
        each(32, lambda i: turned_copy(i, 0).wait_send())


def find_slots(owner_row, block, seg):
    order_ids = jnp.arange(owner_row.shape[0], dtype=jnp.int32)
    mine = owner_row == seg
    rank_of = jnp.sum(jnp.where(mine[None, :] & (order_ids[None, :] < order_ids[:, None]), 1, 0), axis=1)
    matches = mine[None, :] & (rank_of[None, :] == jnp.arange(CAP, dtype=jnp.int32)[:, None])
    tile = jnp.sum(jnp.where(matches, order_ids[None, :], 0), axis=1)[:, None]
    zl, g = block % 2, jnp.arange(BANDS, dtype=jnp.int32)[None, :]
    k, p, q = tile // 16, (tile // 4) % 4, tile % 4
    reach = zl + k
    apart = reach // 2
    row_first = jnp.where(zl == g, 1, 0)
    column_first = jnp.where(reach % 2 == g, 1, 0)
    firsts = row_first + column_first
    whole = jnp.where(firsts == 2, 0, jnp.where(firsts == 0, 2, 3))
    whole = jnp.where(apart == 1, jnp.where(firsts == 2, 1, 4), whole)
    is_whole = jnp.where(apart == 0, 1, jnp.where(apart == 1, column_first, jnp.where(firsts == 2, 1, 0)))
    turned = jnp.where((apart == 2) & (firsts == 0) & (p > q), 1, 0)
    mixed = jnp.where((apart == 2) & (firsts == 1), 1, 0)
    by_row = jnp.where(mixed == 1, 1 - g, turned)
    chunk = jnp.where(by_row == 1, p, q)
    at_x = jnp.where((1 - is_whole) * by_row == 1, q, p)
    at_zh = jnp.where(is_whole == 1, q % 2, jnp.where(apart == 1, 1 - row_first, 1 - mixed))
    at_core = jnp.where(is_whole == 1, q // 2, jnp.where(apart == 1, 0, 1))
    source = at_x * 4 + at_zh * 2 + at_core
    slot = ((zl + g) % 2) * 16 + (source - seg + 16) % 16
    plane = jnp.where(apart == 2, 1 + turned, 0)
    kind = jnp.where(is_whole == 1, jnp.where(apart == 2, 1, 0), 2)
    kind = jnp.where(jnp.sum(jnp.where(matches, 1, 0), axis=1)[:, None] == 1, kind, 3)
    slot = jnp.where(is_whole == 1, slot, plane * 32 + slot)
    place = jnp.where(is_whole == 1, jnp.where(apart == 2, 0, whole), chunk)
    parts = [jnp.broadcast_to(part, (CAP, BANDS)) for part in (kind, slot, place)]
    return jnp.concatenate(parts, axis=1).astype(jnp.int32)


def body(spectra, window_count, tile_owner, phases):
    velocities = phases.shape[2]
    bf16, f32 = jnp.bfloat16, jnp.float32
    dma = pltpu.SemaphoreType.DMA
    return pl.pallas_call(
        kernel,
        out_shape=jax.ShapeDtypeStruct((1, 1, CAP, BANDS, velocities), f32),
        in_specs=[pl.BlockSpec(memory_space=pltpu.VMEM), pl.BlockSpec(memory_space=pltpu.SMEM)] + [pl.BlockSpec(memory_space=pl.ANY)] * 2,
        out_specs=pl.BlockSpec(memory_space=pltpu.VMEM),
        scratch_shapes=[
            pltpu.VMEM((QUAD, 2, TILE, 2 * PART), bf16),
            pltpu.VMEM((QUAD, TILE, 2 * PART), bf16),
            pltpu.VMEM((11, QUAD, TILE, 2 * PART), bf16),
            pltpu.VMEM((ROUNDS, 4, QUAD, TILE, 2 * TILE), bf16),
            pltpu.VMEM((ROUNDS, 2, QUAD, TILE, 2 * TILE), bf16),
            pltpu.VMEM((ROUNDS, 2, TILE, 2 * TILE), bf16),
            pltpu.VMEM((ROUNDS, 2, 2, TILE, 2 * TILE), bf16),
            pltpu.VMEM((ROUNDS, TILE, 2 * TILE), bf16),
            pltpu.VMEM((ROUNDS, TILE, 2 * TILE), bf16),
            pltpu.VMEM((ROUNDS, TILE, 2 * TILE), f32),
            pltpu.VMEM((TILE, velocities), f32),
            pltpu.VMEM((2 * TILE, 2 * velocities), bf16),
            pltpu.VMEM((WHOLE_ROUNDS, 1, velocities), f32),
            pltpu.VMEM((QUAD, 1, velocities), f32),
            pltpu.VMEM((QUAD, 1, velocities), f32),
            pltpu.VMEM((32, NEAR_ROUNDS, 1, velocities), f32),
            pltpu.VMEM((32, 1, 1, velocities), f32),
            pltpu.VMEM((96, QUAD, 1, velocities), f32),
            dma((QUAD,)),
            dma((1,)),
            dma((2, QUAD)),
            dma((2, 2, QUAD)),
            dma((2, 2, QUAD)),
            dma((2, ROUNDS)),
            dma((2, ROUNDS, 2)),
            dma((2, ROUNDS, 2)),
            dma((2, ROUNDS)),
            dma((2, 32)),
            dma((2, 32)),
            dma((2, 96)),
            pltpu.SemaphoreType.REGULAR,
            pltpu.SemaphoreType.REGULAR,
            pltpu.SemaphoreType.REGULAR,
        ],
        compiler_params=pltpu.CompilerParams(vmem_limit_bytes=60 * 1024 * 1024, has_side_effects=True, collective_id=0),
    )(find_slots(tile_owner[0], lax.axis_index("blk"), lax.axis_index("seg")), window_count, spectra[0], phases)


def solution(mesh):
    placed = (P("seg", None, "blk", None), P("seg"), P("blk", None), P())
    return jax.shard_map(
        body,
        mesh=mesh,
        in_specs=placed,
        out_specs=P("blk", "seg", None, None, None),
        check_vma=False,
    )
```
